32 devices in a mesh: rep: 4 (over y, z), vocab: 8 (over x, core).
Axes of the slice: x: 4, y: 2, z: 2, core: 2. Of those that a mesh axis runs over, the one named last changes fastest.
The devices are a block of a 4x4x8 slice.
Arguments:
- hidden: bfloat16 [16384, 2048], P(('rep', 'vocab')), parts along dimension 0
- w_head: bfloat16 [128256, 2048], P('vocab')
- allowed_ids: int32 [8192], P('rep'), parts along dimension 0
- allowed_valid: int32 [8192], P('rep'), parts along dimension 0
- target_pos: int32 [16384], P(('rep', 'vocab')), parts along dimension 0
Outputs:
- output 1: float32 [16384, 2048], P(('rep', 'vocab')), parts along dimension 0
- output 2: float32 [16384], P(('rep', 'vocab')), parts along dimension 0
There are 4 independent parts. The reference program is written for one: setup_inputs(seed, part) draws one part's arguments, and reference() takes and returns one part's arrays. A program takes and returns all parts, laid end to end along the dimension named above; an argument that names none is the same for every part.
All inputs are finite; a program needn't handle non-finite values.
Results may differ from the reference program's by a relative error of at most 0.001.
Values are sent between devices in bfloat16 or wider.
A program may use at most 768 MiB of HBM per device.

```python
import jax
import jax.numpy as jnp
from jax import lax

VOCAB_SIZE = 128256
MODEL_DIM = 2048
LIST_LEN = 2048
BATCH_ROWS = 4096
SHARDS = 8
HEAD_BLOCKS = 128
INV_TEMP = 1.25


def draw_head(key_head):
    block_keys = jax.random.split(key_head, HEAD_BLOCKS)
    row_scale = MODEL_DIM ** -0.5

    def one_block(block_key):
        block_vals = jax.random.normal(block_key, (VOCAB_SIZE // HEAD_BLOCKS, MODEL_DIM), jnp.float32)
        return (block_vals * row_scale).astype(jnp.bfloat16)

    return lax.map(one_block, block_keys).reshape(VOCAB_SIZE, MODEL_DIM)


def draw_list(key_list):
    key_pair, key_move, key_offset, key_order, key_count, key_valid, key_target = jax.random.split(key_list, 7)
    per_shard = LIST_LEN // SHARDS
    slot_cap = 2 * per_shard
    vocab_local = VOCAB_SIZE // SHARDS
    shard_order = jax.random.permutation(key_pair, SHARDS)
    move_sizes = jax.random.randint(key_move, (SHARDS // 2,), 0, per_shard + 1).at[0].set(per_shard)
    shard_gain = jnp.zeros((SHARDS,), jnp.int32).at[shard_order[0::2]].set(move_sizes).at[shard_order[1::2]].set(-move_sizes)
    counts = per_shard + shard_gain
    offset_keys = jax.random.split(key_offset, SHARDS)
    offsets = jax.vmap(lambda one_key: jax.random.permutation(one_key, vocab_local)[:slot_cap])(offset_keys)
    candidates = jnp.arange(SHARDS, dtype=jnp.int32)[:, None] * vocab_local + offsets
    keep_slot = jnp.arange(slot_cap)[None, :] < counts[:, None]
    sort_key = jnp.where(keep_slot, 0, 1) * (SHARDS * slot_cap) + jnp.arange(SHARDS * slot_cap).reshape(SHARDS, slot_cap)
    chosen = jnp.argsort(sort_key.reshape(-1))[:LIST_LEN]
    grouped = candidates.reshape(-1)[chosen]
    allowed_ids = grouped[jax.random.permutation(key_order, LIST_LEN)].astype(jnp.int32)
    valid_count = jax.random.randint(key_count, (), LIST_LEN // 2, LIST_LEN + 1)
    valid_perm = jax.random.permutation(key_valid, LIST_LEN)
    allowed_valid = (valid_perm < valid_count).astype(jnp.int32)
    inverse = jnp.argsort(valid_perm)
    pick_rank = jax.random.randint(key_target, (BATCH_ROWS,), 0, valid_count)
    target_pos = inverse[pick_rank].astype(jnp.int32)
    return allowed_ids, allowed_valid, target_pos


def setup_inputs(seed: int = 0, part: int = 0) -> dict:
    root_key = jax.random.key(seed)
    key_head, key_groups = jax.random.split(root_key)
    key_part = jax.random.fold_in(key_groups, part)
    key_hidden, key_list = jax.random.split(key_part)
    hidden = jax.random.normal(key_hidden, (BATCH_ROWS, MODEL_DIM), jnp.float32).astype(jnp.bfloat16)
    allowed_ids, allowed_valid, target_pos = draw_list(key_list)
    return dict(hidden=hidden, w_head=draw_head(key_head), allowed_ids=allowed_ids, allowed_valid=allowed_valid, target_pos=target_pos)


def reference(hidden, w_head, allowed_ids, allowed_valid, target_pos):
    head_rows = jnp.take(w_head, allowed_ids, axis=0)
    scores = jnp.dot(hidden, head_rows.T, preferred_element_type=jnp.float32) * INV_TEMP
    keep_mask = (allowed_valid > 0)[None, :]
    masked = jnp.where(keep_mask, scores, -jnp.inf)
    log_norm = jax.nn.logsumexp(masked, axis=1)
    token_probs = jnp.where(keep_mask, jnp.exp(masked - log_norm[:, None]), 0.0)
    picked = jnp.take_along_axis(scores, target_pos[:, None], axis=1)[:, 0]
    return token_probs, picked - log_norm
```

```python
import functools

import jax
import jax.numpy as jnp
from jax import lax
from jax.experimental import pallas as pl
from jax.experimental.pallas import tpu as pltpu
from jax.sharding import PartitionSpec as P

INV_TEMP = 1.25
MESH = pl.DeviceIdType.MESH
GROUP = 8
BLOCK = 32
LAG = 128
LANES = 128
LOCAL = 64
STEP = 64
STREAMS = 7


def index_kernel(shards, vocab_local, slot_cap, stream, parts, ids_ref, valid_ref, w_ref, slot_ref, own_ref, cnt_ref,
                 slabs, lid_v, lid_s, sem_s, sems):
    me = lax.axis_index('vocab')
    my_chip, my_core = me // 2, lax.rem(me, 2)
    chips = shards // 2
    list_len = ids_ref.shape[1]
    tiles = list_len // LANES
    ids = ids_ref[...]
    sub = lax.broadcasted_iota(jnp.int32, (shards, list_len), 0)
    rel = ids - sub * vocab_local
    used = valid_ref[...] > 0
    hot = jnp.where((rel >= 0) & (rel < vocab_local) & used, 1.0, 0.0)
    hots = [hot[:, t * LANES:(t + 1) * LANES] for t in range(tiles)]
    stack = jnp.concatenate(hots, axis=0).astype(jnp.bfloat16)
    upper = jnp.where(lax.broadcasted_iota(jnp.int32, (LANES, LANES), 0)
                      <= lax.broadcasted_iota(jnp.int32, (LANES, LANES), 1), 1.0, 0.0).astype(jnp.bfloat16)
    prefix = jnp.dot(stack, upper, preferred_element_type=jnp.float32)
    totals = jnp.dot(stack, jnp.ones((LANES, LANES), jnp.bfloat16), preferred_element_type=jnp.float32)
    carry = jnp.zeros((shards, LANES), jnp.float32)
    ranks = []
    for t in range(tiles):
        seen = prefix[t * shards:(t + 1) * shards] + carry - 1.0
        ranks.append(jnp.sum(hots[t] * seen, axis=0, keepdims=True))
        carry = carry + totals[t * shards:(t + 1) * shards]
    counts = carry.astype(jnp.int32)
    count = [counts[d, 0] for d in range(shards)]
    padded = [(c + (GROUP - 1)) // GROUP * GROUP for c in count]
    both = [padded[2 * c] + padded[2 * c + 1] for c in range(chips)]

    def pick(values, c):
        out = values[0]
        for k in range(1, chips):
            out = jnp.where(c == k, values[k], out)
        return out

    left, right = lax.rem(my_chip + chips - 1, chips), lax.rem(my_chip + 1, chips)
    across = lax.rem(my_chip + 2, chips)
    start_l = jnp.maximum(pick(both, left), LAG)
    start_r = jnp.maximum(pick(both, right), LAG)
    start = [jnp.maximum(b, LAG) for b in both]
    need = both[0]
    for c in range(chips):
        beside = start[(c + 1) % chips] + start[(c + chips - 1) % chips]
        need = jnp.maximum(jnp.maximum(need, both[c]), (beside + both[(c + 2) % chips] + 1) // 2)
    level = sum(jnp.where(need <= stream - STEP * v, 1, 0) for v in range(1, STREAMS))
    length = stream - STEP * level
    base_right = 2 * slot_cap + jnp.where(my_core == 0, 0, stream)
    base_left = 2 * slot_cap + jnp.where(my_core == 0, stream, 0)
    shift_a, limit, shift_b = [], [], []
    for d in range(shards):
        c, e = d // 2, d % 2
        own = c == my_chip
        shift_a.append(jnp.where(own, jnp.where(e == my_core, 0, slot_cap),
                                 base_right + padded[2 * c] - (0 if e else GROUP) + jnp.where(c == left, 0, start_l)))
        limit.append(jnp.where(own | (c == left), 4 * stream + list_len,
                               jnp.where(c == right, 0, base_right + length)))
        shift_b.append(base_left + padded[2 * c + 1] - (GROUP if e else 0) + jnp.where(c == right, 0, start_r))
    down_a = [0.0 if d % 2 else jnp.where(d // 2 == my_chip, 0.0, 2.0 * GROUP) for d in range(shards)]
    down_b = [2.0 * GROUP if d % 2 else 0.0 for d in range(shards)]

    sub1 = lax.broadcasted_iota(jnp.int32, (shards, LANES), 0)

    def column(values):
        out = jnp.zeros((shards, LANES), jnp.float32)
        for d in range(shards):
            out = jnp.where(sub1 == d, values[d] if isinstance(values[d], float) else values[d].astype(jnp.float32), out)
        return out

    columns = [column(v) for v in (shift_a, down_a, limit, shift_b, down_b)]
    slots = []
    for t in range(tiles):
        a, da, lim, b, db = [jnp.sum(hots[t] * col, axis=0, keepdims=True) for col in columns]
        tile = jnp.floor(ranks[t] * (1.0 / GROUP))
        first = a + ranks[t] - da * tile
        slots.append(jnp.where(first < lim, first, b + ranks[t] - db * tile))
    slot_ref[...] = jnp.concatenate(slots, axis=1).astype(jnp.int32) * parts
    mine_pad = [pick([padded[2 * c + e] for c in range(chips)], my_chip) for e in range(2)]
    cnt_ref[0] = jnp.where(my_core == 0, mine_pad[0], mine_pad[1])
    cnt_ref[1] = jnp.where(my_core == 0, mine_pad[1], mine_pad[0])
    cnt_ref[2] = level

    rank = jnp.concatenate(ranks, axis=1).astype(jnp.int32)
    lid = ids - me * vocab_local
    mine = (lid >= 0) & (lid < vocab_local) & used
    rank = jnp.where(mine, rank, -1)
    half = shards // 2
    value = jnp.where(sub < half, lax.shift_right_arithmetic(lid, 7), lid & (LANES - 1)).astype(jnp.float32)
    want = jnp.where(sub < half, sub, sub - half)
    lhs = jnp.where((rank >= 0) & (lax.shift_right_arithmetic(rank, 7) == want), value, 0.0).astype(jnp.bfloat16)
    row = lax.broadcasted_iota(jnp.int32, (LANES, list_len), 0)
    hot_low = jnp.where((rank & (LANES - 1)) == row, 1.0, 0.0).astype(jnp.bfloat16)
    found = lax.dot_general(lhs, hot_low, (((1,), (1,)), ((), ())), preferred_element_type=jnp.float32).astype(jnp.int32)
    local = found[:half] * LANES + found[half:]
    turn = (lax.broadcasted_iota(jnp.int32, local.shape, 1) - local) & (GROUP - 1)
    lid_v[...] = jnp.concatenate([lax.shift_right_arithmetic(local, 3), turn], axis=0)
    copy = pltpu.make_async_copy(lid_v, lid_s, sem_s)
    copy.start()
    copy.wait()

    my_count = count[0]
    for d in range(1, shards):
        my_count = jnp.where(me == d, count[d], my_count)
    per_chunk = 64
    chunks = lax.shift_right_logical(my_count + (per_chunk - 1), 6)

    def fetch(n, _):
        line, lane0 = lax.shift_right_logical(n, 1), (n & 1) * per_chunk

        def some(g, _):
            for i in range(GROUP):
                r = g * GROUP + i
                pltpu.make_async_copy(w_ref.at[lid_s[line, lane0 + r]], slabs.at[n * per_chunk + r], sems.at[n]).start()
            return 0
        return lax.fori_loop(0, per_chunk // GROUP, some, 0)

    lax.fori_loop(0, chunks, fetch, 0)
    lane_row = lax.broadcasted_iota(jnp.int32, own_ref.shape[1:], 0)

    def extract(n, _):
        pltpu.make_async_copy(w_ref.at[pl.ds(0, per_chunk)], slabs.at[pl.ds(n * per_chunk, per_chunk)], sems.at[n]).wait()
        line, lane0 = half + lax.shift_right_logical(n, 1), (n & 1) * per_chunk

        def one(g, _):
            r0 = n * per_chunk + g * GROUP
            acc = jnp.zeros(own_ref.shape[1:], jnp.float32)
            for i in range(GROUP):
                src = slabs[r0 + i].astype(jnp.float32)
                acc = jnp.where(lane_row == i, pltpu.roll(src, lid_s[line, lane0 + g * GROUP + i], 0), acc)
            own_ref[n * (per_chunk // GROUP) + g] = acc.astype(jnp.bfloat16)
            return 0
        return lax.fori_loop(0, per_chunk // GROUP, one, 0, unroll=2)

    lax.fori_loop(0, chunks, extract, 0)


def stream_kernel(shards, slot_cap, stream, longest, cnt_ref, own_ref, hid_ref, out_ref,
                  pool, landed, main, side, outbuf, own_send, own_recv, go_send, go_recv, side_send, side_recv):
    me = lax.axis_index('vocab')
    chips = shards // 2
    my_chip, my_core = me // 2, lax.rem(me, 2)
    partner = me + 1 - 2 * my_core
    ahead = lax.rem(my_chip + jnp.where(my_core == 0, 1, chips - 1), chips) * 2 + my_core
    behind = lax.rem(my_chip + jnp.where(my_core == 0, chips - 1, 1), chips) * 2 + my_core
    barrier = pltpu.get_barrier_semaphore()
    for peer in (partner, ahead, behind):
        pl.semaphore_signal(barrier, inc=1, device_id={'vocab': peer}, device_id_type=MESH)
    pl.semaphore_wait(barrier, 3)

    dim = own_ref.shape[2]
    n_blocks = stream // BLOCK
    lag_blocks = LAG // BLOCK
    tiles = BLOCK // GROUP
    cap_tiles = slot_cap // GROUP
    own_chunks = slot_cap // BLOCK

    def remote(src, dst, send, recv, k, peer):
        at = pl.ds(k * tiles, tiles)
        return pltpu.make_async_remote_copy(src.at[at], dst.at[at], send.at[k], recv.at[k],
                                            device_id={'vocab': peer}, device_id_type=MESH)

    def own_copy(k):
        return remote(own_ref, landed, own_send, own_recv, k, partner)

    def go_copy(k):
        return remote(outbuf, main, go_send, go_recv, k, ahead)

    def side_copy(k):
        return remote(main, side, side_send, side_recv, k, partner)

    for n in range(own_chunks):
        own_copy(n).start()
    first, second = cnt_ref[0], cnt_ref[1]
    both = first + second
    relay = jnp.maximum(both, LAG)

    def send(k):
        for g in range(tiles):
            p = k * BLOCK + g * GROUP
            mine = own_ref[lax.shift_right_logical(jnp.maximum(first - GROUP - p, 0), 3)]
            passed = jnp.where(p < both, p - first, jnp.where(p >= relay, slot_cap + p - relay, 0))
            other = pool[lax.shift_right_logical(jnp.maximum(passed, 0), 3)]
            outbuf[k * tiles + g] = jnp.where(p < first, mine, other)
        go_copy(k).start()

    def take(n):
        own_copy(n).wait_recv()
        pool[pl.ds(n * tiles, tiles)] = landed[pl.ds(n * tiles, tiles)]

    def flat(value):
        return value.reshape(value.shape[0] * GROUP, dim)

    def scores(value):
        return lax.dot_general(value, hid_ref[...], (((1,), (1,)), ((), ())),
                               preferred_element_type=jnp.float32) * INV_TEMP

    def put(got, slot0):
        parts = got.shape[1] // LANES
        for q in range(parts):
            out_ref[pl.ds(slot0 * parts + q, got.shape[0], stride=parts), :] = got[:, q * LANES:(q + 1) * LANES]

    main_slot, side_slot = 2 * slot_cap, 2 * slot_cap + longest
    for k in range(lag_blocks):
        take(k)
        send(k)
    for n in range(lag_blocks, own_chunks):
        take(n)
    local_steps = slot_cap // LOCAL
    local_tiles = LOCAL // GROUP

    def step(a, _):
        go_copy(a).wait_recv()
        side_copy(a).start()
        pool[pl.ds(cap_tiles + a * tiles, tiles)] = main[pl.ds(a * tiles, tiles)]

        @pl.when(a < n_blocks - lag_blocks)
        def _():
            send(a + lag_blocks)

        @pl.when(a >= 2)
        def _():
            b = a - 2
            side_copy(b).wait_recv()
            n = jnp.minimum(b, 2 * local_steps - 1)
            at = pl.ds(lax.rem(n, local_steps) * local_tiles, local_tiles)
            local = jnp.where(n < local_steps, own_ref[at], pool[at])
            got = scores(jnp.concatenate([flat(main[pl.ds(b * tiles, tiles)]), flat(side[pl.ds(b * tiles, tiles)]),
                                          flat(local)], axis=0))
            put(got[:BLOCK], main_slot + b * BLOCK)
            put(got[BLOCK:2 * BLOCK], side_slot + b * BLOCK)
            put(got[2 * BLOCK:], n * LOCAL)

        return 0

    lax.fori_loop(0, n_blocks, step, 0)
    last = n_blocks - 2
    for b in range(last, n_blocks):
        side_copy(b).wait_recv()
    at = pl.ds(last * tiles, 2 * tiles)
    got = scores(jnp.concatenate([flat(main[at]), flat(side[at])], axis=0))
    put(got[:2 * BLOCK], main_slot + last * BLOCK)
    put(got[2 * BLOCK:], side_slot + last * BLOCK)
    for n in range(own_chunks):
        own_copy(n).wait_send()

    def drain(k, _):
        go_copy(k).wait_send()
        side_copy(k).wait_send()
        return 0

    lax.fori_loop(0, n_blocks, drain, 0)


def finish_kernel(slot_ref, st_ref, valid_ref, target_ref, probs_ref, logp_ref, gathered, scores, probs, sems):
    list_len = valid_ref.shape[1]
    parts = target_ref.shape[1] // LANES
    unroll = 32

    def move(g, _):
        for i in range(unroll):
            j = g * unroll + i
            gathered[pl.ds(pl.multiple_of(j * parts, parts), parts), :] = st_ref[pl.ds(pl.multiple_of(slot_ref[0, j], parts), parts), :]
        return 0

    lax.fori_loop(0, list_len // unroll, move, 0)
    valid = valid_ref[...] > 0
    sub = lax.broadcasted_iota(jnp.int32, (LANES, LANES), 0)

    def put(q):
        return pltpu.make_async_copy(probs.at[q], probs_ref.at[pl.ds(pl.multiple_of(q * LANES, LANES), LANES), :], sems.at[q])

    def part(q, _):
        at = pl.ds(pl.multiple_of(q * LANES, LANES), LANES)
        target = target_ref[:, at]
        picked = jnp.zeros((LANES, LANES), jnp.float32)
        for t in range(list_len // LANES):
            x = gathered[pl.ds(t * LANES * parts + q, LANES, stride=parts), :]
            picked = picked + jnp.where(sub == target - t * LANES, x, 0.0)
            scores[:, t * LANES:(t + 1) * LANES] = x.T
        s = scores[...]
        top = jnp.max(jnp.where(valid, s, -jnp.inf), axis=1, keepdims=True)
        e = jnp.where(valid, jnp.exp(s - top), 0.0)
        total = jnp.sum(e, axis=1, keepdims=True)
        probs[q] = e * (1.0 / total)
        put(q).start()
        lse = jnp.broadcast_to(top + jnp.log(total), (LANES, LANES)).T
        logp_ref[:, at] = jnp.sum(picked, axis=0, keepdims=True) - lse[:1]
        return 0

    lax.fori_loop(0, parts, part, 0)
    for q in range(parts):
        put(q).wait()


def solution(mesh):
    shards = mesh.shape['vocab']
    chips = shards // 2
    assert chips == 4

    def device_step(hidden, w_head, allowed_ids, allowed_valid, target_pos):
        list_len = allowed_ids.shape[0]
        rows, dim = hidden.shape
        vocab_local = w_head.shape[0]
        slot_cap = 2 * list_len // shards
        stream = list_len // 2 + LAG // 2
        total_slots = 2 * slot_cap + 2 * stream
        vmem = pl.BlockSpec(memory_space=pltpu.VMEM)
        smem = pl.BlockSpec(memory_space=pltpu.SMEM)
        tile_rows = slot_cap // GROUP
        slot, own, cnt = pl.pallas_call(
            functools.partial(index_kernel, shards, vocab_local, slot_cap, stream, rows // LANES),
            out_shape=(jax.ShapeDtypeStruct((1, list_len), jnp.int32),
                       jax.ShapeDtypeStruct((tile_rows, GROUP, dim), jnp.bfloat16),
                       jax.ShapeDtypeStruct((3,), jnp.int32)),
            in_specs=[vmem, vmem, pl.BlockSpec(memory_space=pl.ANY)],
            out_specs=(vmem, vmem, smem),
            scratch_shapes=[
                pltpu.VMEM((slot_cap, GROUP, dim), jnp.bfloat16),
                pltpu.VMEM((shards, LANES), jnp.int32),
                pltpu.SMEM((shards, LANES), jnp.int32),
                pltpu.SemaphoreType.DMA,
                pltpu.SemaphoreType.DMA((slot_cap // 64,)),
            ],
            compiler_params=pltpu.CompilerParams(vmem_limit_bytes=32 * 2**20),
            name='index',
        )(allowed_ids.reshape(1, list_len), allowed_valid.reshape(1, list_len), w_head.reshape(vocab_local // GROUP, GROUP, dim))

        def streamer(level):
            length = stream - STEP * level
            n_blocks, tiles = length // BLOCK, length // GROUP
            return pl.pallas_call(
                functools.partial(stream_kernel, shards, slot_cap, length, stream),
                out_shape=jax.ShapeDtypeStruct((total_slots * rows // LANES, LANES), jnp.float32),
                in_specs=[smem, vmem, vmem],
                out_specs=vmem,
                scratch_shapes=[
                    pltpu.VMEM((tile_rows + tiles, GROUP, dim), jnp.bfloat16),
                    pltpu.VMEM((tile_rows, GROUP, dim), jnp.bfloat16),
                    pltpu.VMEM((tiles, GROUP, dim), jnp.bfloat16),
                    pltpu.VMEM((tiles, GROUP, dim), jnp.bfloat16),
                    pltpu.VMEM((tiles, GROUP, dim), jnp.bfloat16),
                    pltpu.SemaphoreType.DMA((slot_cap // BLOCK,)),
                    pltpu.SemaphoreType.DMA((slot_cap // BLOCK,)),
                    pltpu.SemaphoreType.DMA((n_blocks,)),
                    pltpu.SemaphoreType.DMA((n_blocks,)),
                    pltpu.SemaphoreType.DMA((n_blocks,)),
                    pltpu.SemaphoreType.DMA((n_blocks,)),
                ],
                compiler_params=pltpu.CompilerParams(
                    collective_id=level, has_side_effects=True, vmem_limit_bytes=32 * 2**20),
                name='stream%d' % length,
            )

        finish = pl.pallas_call(
            finish_kernel,
            out_shape=(jax.ShapeDtypeStruct((rows, list_len), jnp.float32),
                       jax.ShapeDtypeStruct((1, rows), jnp.float32)),
            in_specs=[smem, vmem, vmem, vmem],
            out_specs=(pl.BlockSpec(memory_space=pl.ANY), vmem),
            scratch_shapes=[
                pltpu.VMEM((list_len * rows // LANES, LANES), jnp.float32),
                pltpu.VMEM((LANES, list_len), jnp.float32),
                pltpu.VMEM((rows // LANES, LANES, list_len), jnp.float32),
                pltpu.SemaphoreType.DMA((rows // LANES,)),
            ],
            compiler_params=pltpu.CompilerParams(vmem_limit_bytes=32 * 2**20),
            name='finish',
        )

        def branch(level):
            return lambda slot, cnt, own, hidden, valid, target: finish(slot, streamer(level)(cnt, own, hidden), valid, target)

        probs, logp = lax.switch(cnt[2], [branch(v) for v in range(STREAMS)], slot, cnt, own, hidden,
                                 allowed_valid.reshape(1, list_len), target_pos.reshape(1, rows))
        return probs, logp.reshape(rows)

    row_spec = P(('rep', 'vocab'))
    mat_spec = P(('rep', 'vocab'), None)
    return jax.shard_map(device_step, mesh=mesh, in_specs=(mat_spec, P('vocab', None), P('rep'), P('rep'), row_spec),
                         out_specs=(mat_spec, row_spec), check_vma=False)
```

```python
import functools

import jax
import jax.numpy as jnp
from jax import lax
from jax.experimental import pallas as pl
from jax.experimental.pallas import tpu as pltpu
from jax.sharding import PartitionSpec as P

INV_TEMP = 1.25
MESH = pl.DeviceIdType.MESH
GROUP = 8
BLOCK = 32
ALONE = 32
LAG = 128
LANES = 128
LOCAL = 64
STEP = 32
STREAMS = 13


def index_kernel(shards, vocab_local, slot_cap, stream, parts, ids_ref, valid_ref, w_ref, slot_ref, pair_ref, hot_ref, cnt_ref, level_ref,
                 lid_v, lid_s, sem_s, sems):
    me = lax.axis_index('vocab')
    my_chip, my_core = me // 2, lax.rem(me, 2)
    chips = shards // 2
    list_len = ids_ref.shape[1]
    tiles = list_len // LANES
    ids = ids_ref[...]
    sub = lax.broadcasted_iota(jnp.int32, (shards, list_len), 0)
    rel = ids - sub * vocab_local
    used = valid_ref[...] > 0
    hot = jnp.where((rel >= 0) & (rel < vocab_local) & used, 1.0, 0.0)
    hots = [hot[:, t * LANES:(t + 1) * LANES] for t in range(tiles)]
    stack = jnp.concatenate(hots, axis=0).astype(jnp.bfloat16)
    upper = jnp.where(lax.broadcasted_iota(jnp.int32, (LANES, LANES), 0)
                      <= lax.broadcasted_iota(jnp.int32, (LANES, LANES), 1), 1.0, 0.0).astype(jnp.bfloat16)
    prefix = jnp.dot(stack, upper, preferred_element_type=jnp.float32)
    totals = jnp.dot(stack, jnp.ones((LANES, LANES), jnp.bfloat16), preferred_element_type=jnp.float32)
    carry = jnp.zeros((shards, LANES), jnp.float32)
    ranks = []
    for t in range(tiles):
        seen = prefix[t * shards:(t + 1) * shards] + carry - 1.0
        ranks.append(jnp.sum(hots[t] * seen, axis=0, keepdims=True))
        carry = carry + totals[t * shards:(t + 1) * shards]
    counts = carry.astype(jnp.int32)
    count = [counts[d, 0] for d in range(shards)]
    padded = [(c + (GROUP - 1)) // GROUP * GROUP for c in count]
    both = [padded[2 * c] + padded[2 * c + 1] for c in range(chips)]

    def pick(values, c):
        out = values[0]
        for k in range(1, chips):
            out = jnp.where(c == k, values[k], out)
        return out

    left, right = lax.rem(my_chip + chips - 1, chips), lax.rem(my_chip + 1, chips)
    across = lax.rem(my_chip + 2, chips)
    next_r = [jnp.maximum(padded[2 * c], ALONE) for c in range(chips)]
    next_l = [jnp.maximum(padded[2 * c + 1], ALONE) for c in range(chips)]
    end_r = [next_r[c] + padded[2 * c + 1] for c in range(chips)]
    end_l = [next_l[c] + padded[2 * c] for c in range(chips)]
    start_r = [jnp.maximum(e, LAG) for e in end_r]
    start_l = [jnp.maximum(e, LAG) for e in end_l]
    need = end_r[0]
    for c in range(chips):
        span = end_r[c] + end_l[c] - both[c]
        beside = start_r[(c + 2 - 1) % chips] + start_l[(c + 2 + 1) % chips]
        need = jnp.maximum(jnp.maximum(need, jnp.maximum(end_r[c], end_l[c])), lax.shift_right_logical(beside + span + 1, 1))
    level = sum(jnp.where(need <= stream - STEP * v, 1, 0) for v in range(1, STREAMS))
    length = stream - STEP * level
    base_right = 2 * slot_cap + jnp.where(my_core == 0, 0, stream)
    base_left = 2 * slot_cap + jnp.where(my_core == 0, stream, 0)
    relay_r, relay_l = pick(start_r, left), pick(start_l, right)
    shift_a, limit, shift_b = [], [], []
    for d in range(shards):
        c, e = d // 2, d % 2
        own = c == my_chip
        first_r = next_r[c] if e else padded[2 * c] - GROUP
        first_l = padded[2 * c + 1] - GROUP if e else next_l[c]
        shift_a.append(jnp.where(own, jnp.where(e == my_core, 0, slot_cap),
                                 base_right + first_r + jnp.where(c == left, 0, relay_r)))
        limit.append(jnp.where(own | (c == left), 4 * stream + list_len,
                               jnp.where(c == right, 0, base_right + length)))
        shift_b.append(base_left + first_l + jnp.where(c == right, 0, relay_l))
    down_a = [0.0 if d % 2 else jnp.where(d // 2 == my_chip, 0.0, 2.0 * GROUP) for d in range(shards)]
    down_b = [2.0 * GROUP if d % 2 else 0.0 for d in range(shards)]

    sub1 = lax.broadcasted_iota(jnp.int32, (shards, LANES), 0)

    def column(values):
        out = jnp.zeros((shards, LANES), jnp.float32)
        for d in range(shards):
            out = jnp.where(sub1 == d, values[d] if isinstance(values[d], float) else values[d].astype(jnp.float32), out)
        return out

    rank = jnp.concatenate(ranks, axis=1).astype(jnp.int32)
    lid = ids - me * vocab_local
    mine = (lid >= 0) & (lid < vocab_local) & used
    rank = jnp.where(mine, rank, -1)
    half = shards // 2
    value = jnp.where(sub < half, lax.shift_right_arithmetic(lid, 7), lid & (LANES - 1)).astype(jnp.float32)
    want = jnp.where(sub < half, sub, sub - half)
    lhs = jnp.where((rank >= 0) & (lax.shift_right_arithmetic(rank, 7) == want), value, 0.0).astype(jnp.bfloat16)
    row = lax.broadcasted_iota(jnp.int32, (LANES, list_len), 0)
    hot_low = jnp.where((rank & (LANES - 1)) == row, 1.0, 0.0).astype(jnp.bfloat16)
    found = lax.dot_general(lhs, hot_low, (((1,), (1,)), ((), ())), preferred_element_type=jnp.float32).astype(jnp.int32)
    local = found[:half] * LANES + found[half:]
    lid_v[...] = jnp.concatenate([lax.shift_right_arithmetic(local, 1), local & 1], axis=0)
    copy = pltpu.make_async_copy(lid_v, lid_s, sem_s)
    copy.start()
    columns = [column(v) for v in (shift_a, down_a, limit, shift_b, down_b)]
    slots = []
    for t in range(tiles):
        a, da, lim, b, db = [jnp.sum(hots[t] * col, axis=0, keepdims=True) for col in columns]
        tile = jnp.floor(ranks[t] * (1.0 / GROUP))
        first = a + ranks[t] - da * tile
        slots.append(jnp.where(first < lim, first, b + ranks[t] - db * tile))
    slot_ref[...] = jnp.concatenate(slots, axis=1).astype(jnp.int32) * parts
    mine_pad = [pick([padded[2 * c + e] for c in range(chips)], my_chip) for e in range(2)]
    cnt_ref[0] = jnp.where(my_core == 0, mine_pad[0], mine_pad[1])
    cnt_ref[1] = jnp.where(my_core == 0, mine_pad[1], mine_pad[0])
    level_ref[0] = level

    copy.wait()
    my_count = count[0]
    for d in range(1, shards):
        my_count = jnp.where(me == d, count[d], my_count)
    chunks = lax.shift_right_logical(my_count + (LANES - 1), 7)

    def fetch(n, _):
        def some(g, _):
            for i in range(GROUP):
                r = g * GROUP + i
                pair = lid_s[n, r]
                pltpu.make_async_copy(w_ref.at[lax.shift_right_logical(pair, 2), :, pl.ds(pair & 3, 1)],
                                      pair_ref.at[:, pl.ds(n * LANES + r, 1)], sems.at[n]).start()
            return 0
        return lax.fori_loop(0, LANES // GROUP, some, 0)

    lax.fori_loop(0, chunks, fetch, 0)
    odd = jnp.concatenate([local & 1, local & 1], axis=0).astype(jnp.float32).T
    spot = lax.broadcasted_iota(jnp.int32, (LANES, 2 * LANES), 1) - 2 * lax.broadcasted_iota(jnp.int32, (LANES, 2 * LANES), 0)
    for n in range(half):
        hot_ref[n] = jnp.where(spot.astype(jnp.float32) == odd[:, n:n + 1], 1.0, 0.0).astype(jnp.bfloat16)

    def settle(n, _):
        at = pl.ds(n * LANES, LANES)
        pltpu.make_async_copy(pair_ref.at[:, at], pair_ref.at[:, at], sems.at[n]).wait()
        return 0

    lax.fori_loop(0, chunks, settle, 0)


def stream_kernel(shards, slot_cap, stream, longest, cnt_ref, hot_ref, pair_ref, hid_ref, out_ref,
                  own_ref, pool, landed, main, side, outbuf, own_send, own_recv, go_send, go_recv, side_send, side_recv):
    me = lax.axis_index('vocab')
    chips = shards // 2
    my_chip, my_core = me // 2, lax.rem(me, 2)
    partner = me + 1 - 2 * my_core
    ahead = lax.rem(my_chip + jnp.where(my_core == 0, 1, chips - 1), chips) * 2 + my_core
    behind = lax.rem(my_chip + jnp.where(my_core == 0, chips - 1, 1), chips) * 2 + my_core
    barrier = pltpu.get_barrier_semaphore()
    for peer in (partner, ahead, behind):
        pl.semaphore_signal(barrier, inc=1, device_id={'vocab': peer}, device_id_type=MESH)
    dim = own_ref.shape[2]

    def choose(n, _):
        for c in range(0, pair_ref.shape[0], 2):
            at = pl.ds(pl.multiple_of(n * 2 * LANES, 2 * LANES), 2 * LANES)
            got = jnp.dot(hot_ref[n], jnp.concatenate([pair_ref[c, at], pair_ref[c + 1, at]], axis=1),
                          preferred_element_type=jnp.float32).astype(jnp.bfloat16)
            own_ref[pl.ds(n * (LANES // GROUP), LANES // GROUP), :, c * LANES:(c + 2) * LANES] = got.reshape(
                LANES // GROUP, GROUP, 2 * LANES)
        return 0

    lax.fori_loop(0, hot_ref.shape[0], choose, 0)
    pl.semaphore_wait(barrier, 3)

    n_blocks = stream // BLOCK
    lag_blocks = LAG // BLOCK
    tiles = BLOCK // GROUP
    cap_tiles = slot_cap // GROUP
    chunks = [(k * tiles, tiles) for k in range(lag_blocks)]
    rest = lag_blocks * tiles
    while rest < cap_tiles:
        chunks.append((rest, min(16, cap_tiles - rest)))
        rest += 16

    def remote(src, dst, send, recv, at, peer):
        return pltpu.make_async_remote_copy(src.at[at], dst.at[at], send, recv,
                                            device_id={'vocab': peer}, device_id_type=MESH)

    def own_copy(n):
        return remote(own_ref, landed, own_send, own_recv.at[n], pl.ds(*chunks[n]), partner)

    def go_copy(k):
        return remote(outbuf, main, go_send, go_recv.at[k], pl.ds(k * tiles, tiles), ahead)

    def side_copy(k):
        return remote(main, side, side_send, side_recv.at[k], pl.ds(k * tiles, tiles), partner)

    first, second = cnt_ref[0], cnt_ref[1]
    begin = jnp.maximum(first, ALONE)
    both = begin + second
    relay = jnp.maximum(both, LAG)

    def mine(p):
        return own_ref[lax.shift_right_logical(jnp.maximum(first - GROUP - p, 0), 3)]

    def send(k):
        for g in range(tiles):
            p = k * BLOCK + g * GROUP
            passed = jnp.where(p < both, p - begin, jnp.where(p >= relay, slot_cap + p - relay, 0))
            other = pool[lax.shift_right_logical(jnp.maximum(passed, 0), 3)]
            outbuf[k * tiles + g] = jnp.where(p < first, mine(p), other)
        go_copy(k).start()

    def take(n):
        own_copy(n).wait_recv()
        at = pl.ds(*chunks[n])
        pool[at] = landed[at]

    own_copy(0).start()
    for g in range(tiles):
        outbuf[g] = mine(g * GROUP)
    go_copy(0).start()
    for n in range(1, len(chunks)):
        own_copy(n).start()

    def flat(value):
        return value.reshape(value.shape[0] * GROUP, dim)

    def scores(value):
        return lax.dot_general(value, hid_ref[...], (((1,), (1,)), ((), ())),
                               preferred_element_type=jnp.float32) * INV_TEMP

    def put(got, slot0):
        parts = got.shape[1] // LANES
        for q in range(parts):
            out_ref[pl.ds(slot0 * parts + q, got.shape[0], stride=parts), :] = got[:, q * LANES:(q + 1) * LANES]

    main_slot, side_slot = 2 * slot_cap, 2 * slot_cap + longest
    for k in range(1, lag_blocks):
        take(k - 1)
        send(k)
    for n in range(lag_blocks - 1, len(chunks)):
        take(n)
    local_steps = slot_cap // LOCAL
    local_tiles = LOCAL // GROUP

    def step(a, _):
        go_copy(a).wait_recv()
        side_copy(a).start()
        pool[pl.ds(cap_tiles + a * tiles, tiles)] = main[pl.ds(a * tiles, tiles)]

        @pl.when(a < n_blocks - lag_blocks)
        def _():
            send(a + lag_blocks)

        @pl.when(a >= 2)
        def _():
            b = a - 2
            side_copy(b).wait_recv()
            n = jnp.minimum(b, 2 * local_steps - 1)
            at = pl.ds(lax.rem(n, local_steps) * local_tiles, local_tiles)
            local = jnp.where(n < local_steps, own_ref[at], pool[at])
            got = scores(jnp.concatenate([flat(main[pl.ds(b * tiles, tiles)]), flat(side[pl.ds(b * tiles, tiles)]),
                                          flat(local)], axis=0))
            put(got[:BLOCK], main_slot + b * BLOCK)
            put(got[BLOCK:2 * BLOCK], side_slot + b * BLOCK)
            put(got[2 * BLOCK:], n * LOCAL)

        return 0

    lax.fori_loop(0, n_blocks, step, 0)
    last = n_blocks - 2
    for b in range(last, n_blocks):
        side_copy(b).wait_recv()
    at = pl.ds(last * tiles, 2 * tiles)
    got = scores(jnp.concatenate([flat(main[at]), flat(side[at])], axis=0))
    put(got[:2 * BLOCK], main_slot + last * BLOCK)
    put(got[2 * BLOCK:], side_slot + last * BLOCK)
    remote(own_ref, landed, own_send, own_recv.at[0], pl.ds(0, cap_tiles), partner).wait_send()
    remote(outbuf, main, go_send, go_recv.at[0], pl.ds(0, n_blocks * tiles), ahead).wait_send()
    remote(main, side, side_send, side_recv.at[0], pl.ds(0, n_blocks * tiles), partner).wait_send()


def finish_kernel(slot_ref, st_ref, valid_ref, target_ref, probs_ref, logp_ref, gathered, scores, probs, slot_s, sems, slot_sems):
    list_len = valid_ref.shape[1]
    parts = target_ref.shape[1] // LANES
    unroll = 32

    pieces = slot_sems.shape[0]
    piece = list_len // pieces

    def table(n):
        at = pl.ds(n * piece, piece)
        return pltpu.make_async_copy(slot_ref.at[:, at], slot_s.at[:, at], slot_sems.at[n])

    for n in range(pieces):
        table(n).start()

    def move(g, _):
        @pl.when(lax.rem(g, piece // unroll) == 0)
        def _():
            at = pl.ds(pl.multiple_of(g * unroll, piece), piece)
            pltpu.make_async_copy(slot_ref.at[:, at], slot_s.at[:, at], slot_sems.at[g // (piece // unroll)]).wait()

        for i in range(unroll):
            j = g * unroll + i
            gathered[pl.ds(pl.multiple_of(j * parts, parts), parts), :] = st_ref[pl.ds(pl.multiple_of(slot_s[0, j], parts), parts), :]
        return 0

    lax.fori_loop(0, list_len // unroll, move, 0)
    valid = valid_ref[...] > 0
    sub = lax.broadcasted_iota(jnp.int32, (LANES, LANES), 0)

    def put(q):
        return pltpu.make_async_copy(probs.at[q], probs_ref.at[pl.ds(pl.multiple_of(q * LANES, LANES), LANES), :], sems.at[q])

    def part(q, _):
        at = pl.ds(pl.multiple_of(q * LANES, LANES), LANES)
        target = target_ref[:, at]
        picked = jnp.zeros((LANES, LANES), jnp.float32)
        for t in range(list_len // LANES):
            x = gathered[pl.ds(t * LANES * parts + q, LANES, stride=parts), :]
            picked = picked + jnp.where(sub == target - t * LANES, x, 0.0)
            scores[:, t * LANES:(t + 1) * LANES] = x.T
        s = scores[...]
        top = jnp.max(jnp.where(valid, s, -jnp.inf), axis=1, keepdims=True)
        e = jnp.where(valid, jnp.exp(s - top), 0.0)
        total = jnp.sum(e, axis=1, keepdims=True)
        probs[q] = e * (1.0 / total)
        put(q).start()
        lse = jnp.broadcast_to(top + jnp.log(total), (LANES, LANES)).T
        logp_ref[:, at] = jnp.sum(picked, axis=0, keepdims=True) - lse[:1]
        return 0

    lax.fori_loop(0, parts, part, 0)
    for q in range(parts):
        put(q).wait()


def solution(mesh):
    shards = mesh.shape['vocab']
    chips = shards // 2
    assert chips == 4

    def device_step(hidden, w_head, allowed_ids, allowed_valid, target_pos):
        list_len = allowed_ids.shape[0]
        rows, dim = hidden.shape
        vocab_local = w_head.shape[0]
        slot_cap = 2 * list_len // shards
        stream = list_len // 2 + LAG // 2
        total_slots = 2 * slot_cap + 2 * stream
        tile_rows = slot_cap // GROUP
        vmem = pl.BlockSpec(memory_space=pltpu.VMEM)
        smem = pl.BlockSpec(memory_space=pltpu.SMEM)
        halves, wide = shards // 2, dim // LANES
        any_space = pl.BlockSpec(memory_space=pl.ANY)
        pairs = w_head.reshape(vocab_local // GROUP, GROUP // 2, 2, wide, LANES).transpose(0, 3, 1, 2, 4)
        slot, pair, hot, cnt, level = pl.pallas_call(
            functools.partial(index_kernel, shards, vocab_local, slot_cap, stream, rows // LANES),
            out_shape=(jax.ShapeDtypeStruct((1, list_len), jnp.int32),
                       jax.ShapeDtypeStruct((wide, slot_cap, 2, LANES), jnp.bfloat16),
                       jax.ShapeDtypeStruct((halves, LANES, 2 * LANES), jnp.bfloat16),
                       jax.ShapeDtypeStruct((2,), jnp.int32),
                       jax.ShapeDtypeStruct((1,), jnp.int32)),
            in_specs=[vmem, vmem, any_space],
            out_specs=(vmem, vmem, vmem, smem, smem),
            scratch_shapes=[
                pltpu.VMEM((shards, LANES), jnp.int32),
                pltpu.SMEM((shards, LANES), jnp.int32),
                pltpu.SemaphoreType.DMA,
                pltpu.SemaphoreType.DMA((halves,)),
            ],
            compiler_params=pltpu.CompilerParams(vmem_limit_bytes=16 * 2**20),
            name='index',
        )(allowed_ids.reshape(1, list_len), allowed_valid.reshape(1, list_len), pairs)
        pair = pair.reshape(wide, 2 * slot_cap, LANES)

        def streamer(level):
            length = stream - STEP * level
            n_blocks, tiles = length // BLOCK, length // GROUP
            return pl.pallas_call(
                functools.partial(stream_kernel, shards, slot_cap, length, stream),
                out_shape=jax.ShapeDtypeStruct((total_slots * rows // LANES, LANES), jnp.float32),
                in_specs=[smem, vmem, vmem, vmem],
                out_specs=vmem,
                scratch_shapes=[
                    pltpu.VMEM((tile_rows, GROUP, dim), jnp.bfloat16),
                    pltpu.VMEM((tile_rows + tiles, GROUP, dim), jnp.bfloat16),
                    pltpu.VMEM((tile_rows, GROUP, dim), jnp.bfloat16),
                    pltpu.VMEM((tiles, GROUP, dim), jnp.bfloat16),
                    pltpu.VMEM((tiles, GROUP, dim), jnp.bfloat16),
                    pltpu.VMEM((tiles, GROUP, dim), jnp.bfloat16),
                    pltpu.SemaphoreType.DMA,
                    pltpu.SemaphoreType.DMA((LAG // BLOCK + (slot_cap - LAG) // LANES,)),
                    pltpu.SemaphoreType.DMA,
                    pltpu.SemaphoreType.DMA((n_blocks,)),
                    pltpu.SemaphoreType.DMA,
                    pltpu.SemaphoreType.DMA((n_blocks,)),
                ],
                compiler_params=pltpu.CompilerParams(
                    collective_id=level, has_side_effects=True, vmem_limit_bytes=32 * 2**20),
                name='stream%d' % length,
            )

        finish = pl.pallas_call(
            finish_kernel,
            out_shape=(jax.ShapeDtypeStruct((rows, list_len), jnp.float32),
                       jax.ShapeDtypeStruct((1, rows), jnp.float32)),
            in_specs=[any_space, vmem, vmem, vmem],
            out_specs=(any_space, vmem),
            scratch_shapes=[
                pltpu.VMEM((list_len * rows // LANES, LANES), jnp.float32),
                pltpu.VMEM((LANES, list_len), jnp.float32),
                pltpu.VMEM((rows // LANES, LANES, list_len), jnp.float32),
                pltpu.SMEM((1, list_len), jnp.int32),
                pltpu.SemaphoreType.DMA((rows // LANES,)),
                pltpu.SemaphoreType.DMA((8,)),
            ],
            compiler_params=pltpu.CompilerParams(vmem_limit_bytes=32 * 2**20),
            name='finish',
        )

        def branch(level):
            return lambda slot, cnt, hot, pair, hidden, valid, target: finish(slot, streamer(level)(cnt, hot, pair, hidden), valid, target)

        probs, logp = lax.switch(level[0], [branch(v) for v in range(STREAMS)], slot, cnt, hot, pair, hidden,
                                 allowed_valid.reshape(1, list_len), target_pos.reshape(1, rows))
        return probs, logp.reshape(rows)

    row_spec = P(('rep', 'vocab'))
    mat_spec = P(('rep', 'vocab'), None)
    return jax.shard_map(device_step, mesh=mesh, in_specs=(mat_spec, P('vocab', None), P('rep'), P('rep'), row_spec),
                         out_specs=(mat_spec, row_spec), check_vma=False)
```
